256 devices in a mesh: seq: 4 (over y_hi, core), blk: 64 (over z, x, y_lo).
Axes of the slice: x: 4, y: 4 (y_hi: 2, y_lo: 2; y = y_hi * 2 + y_lo), z: 8, core: 2. Of those that a mesh axis runs over, the one named last changes fastest.
Arguments:
- kv_cache: bfloat16 [4, 2, 16, 4096, 1024], P(None, None, None, ('seq', 'blk')), may hold values from -18 to 18, as said below
- queries: bfloat16 [4, 128, 1024], P(None, 'blk'), may hold values from -400 to 400
- fresh_key_value: bfloat16 [4, 2, 128, 128], P(None, None, 'blk'), may hold values from -70 to 70
- lengths: int32 [16], replicated, may hold values from 1 to 4096, 49152 in all
Outputs:
- quant_cache: bfloat16 [4, 2, 128, 4096, 128], P(None, None, 'blk', 'seq')
- block_scale: float32 [4, 2, 128, 32], P(None, None, 'blk', 'seq')
- attended: bfloat16 [4, 128, 1024], P(None, 'blk')
The draws below stay inside these ranges and needn't reach their ends.
Inputs may be any that keep to these rules, and one draw needn't show every extreme that they name: `kv_cache`: each entry is a random value times a factor drawn for its position and head. `lengths`: every sequence has at least one live position, and some sequence uses all 4096.
All inputs are finite; a program needn't handle non-finite values.
Results may differ from the reference program's by a relative error of at most 0.003.
The reference program's roundings to bfloat16 on the way count: a program that leaves them out, or rounds other values in their place, can miss the bound.
Values may be sent and summed in bfloat16 or wider, within the bound.
A program may use at most 64 MiB of HBM per device.

```python
import math
import jax
import jax.numpy as jnp
import numpy as np
from jax import lax

KEY_VALUE_HEADS = 8
HEAD_DIM = 128
QUERY_GROUP = 8
SEQUENCE_COUNT = 16
CACHE_LENGTH = 4096
LAYER_COUNT = 4
BLOCK = 128


def draw_kv_cache(key, part):
    first_part, second_part = jax.random.split(jax.random.fold_in(key, 11))
    array_shape = (LAYER_COUNT, 2, SEQUENCE_COUNT, CACHE_LENGTH, KEY_VALUE_HEADS, HEAD_DIM)
    base_offset = jax.random.truncated_normal(first_part, -4.0, 4.0, array_shape, jnp.float32)
    scale_factor = jnp.exp(jax.random.uniform(second_part, (LAYER_COUNT, 2, SEQUENCE_COUNT, CACHE_LENGTH, KEY_VALUE_HEADS, 1), jnp.float32, -1.5, 1.5))
    return (base_offset * scale_factor).reshape(LAYER_COUNT, 2, SEQUENCE_COUNT, CACHE_LENGTH, KEY_VALUE_HEADS * HEAD_DIM).astype(jnp.bfloat16)


def draw_queries(key, part):
    first_part, second_part = jax.random.split(jax.random.fold_in(key, 23))
    base_offset = jax.random.truncated_normal(first_part, -6.0, 6.0, (LAYER_COUNT, KEY_VALUE_HEADS * SEQUENCE_COUNT, QUERY_GROUP, HEAD_DIM), jnp.float32)
    return base_offset.reshape(LAYER_COUNT, KEY_VALUE_HEADS * SEQUENCE_COUNT, QUERY_GROUP * HEAD_DIM).astype(jnp.bfloat16)


def draw_fresh_key_value(key, part):
    noise_key, value_key = jax.random.split(jax.random.fold_in(key, 37))
    query_rows = draw_queries(key, part).astype(jnp.float32)
    query_rows = query_rows.reshape(LAYER_COUNT, KEY_VALUE_HEADS * SEQUENCE_COUNT, QUERY_GROUP, HEAD_DIM)
    summed = jnp.sum(query_rows, axis=2)
    length = jnp.sqrt(jnp.sum(summed * summed, axis=-1, keepdims=True) + 1.0)
    noise = 0.5 * jax.random.normal(noise_key, summed.shape, jnp.float32)
    fresh_key = jnp.clip(5.0 * jnp.sqrt(jnp.float32(HEAD_DIM)) * summed / length + noise, -70.0, 70.0)
    fresh_value = jax.random.truncated_normal(value_key, -6.0, 6.0, summed.shape, jnp.float32)
    return jnp.stack([fresh_key, fresh_value], axis=1).astype(jnp.bfloat16)


def length_profile(number_of, total, limit, skew):
    weights = [(1 << 20) // math.isqrt(rank ** skew) + 1 for rank in range(2, number_of + 1)]
    spare, counts = total - limit - (number_of - 1), [1] * (number_of - 1)
    while spare > 0:
        candidates = [i for i in range(number_of - 1) if counts[i] < limit]
        pool, left = sum([weights[i] for i in candidates]), spare
        for i in candidates:
            more = min(limit - counts[i], max(1, left * weights[i] // pool), spare)
            counts[i] = counts[i] + more
            spare = spare - more
    return np.array([limit] + counts)


def ragged(stream_key, amount, total, reach, slope):
    if amount == 2:
        one = jax.random.randint(stream_key, (), max(1, total - reach), min(reach, total - 1) + 1)
        return jnp.stack([one, total - one])
    tallies = jnp.asarray(length_profile(amount, total, reach, slope), jnp.int32)
    pairs = (amount - 1) // 2
    source_of, taker = tallies[1:1 + 2 * pairs:2], tallies[2:2 + 2 * pairs:2]
    margin = jnp.minimum(source_of - 1, reach - taker)
    moved = jax.random.randint(jax.random.fold_in(stream_key, 1), (pairs,), 0, 1 << 20) % (margin + 1)
    tallies = tallies.at[1:1 + 2 * pairs:2].set(source_of - moved).at[2:2 + 2 * pairs:2].set(taker + moved)
    return tallies[jax.random.permutation(jax.random.fold_in(stream_key, 2), amount)]


def setup_inputs(seed: int = 0) -> dict:
    key_list = jax.random.split(jax.random.key(seed), 5)
    return {
        "kv_cache": draw_kv_cache(jax.random.fold_in(key_list[4], 71), 0),
        "queries": draw_queries(jax.random.fold_in(key_list[4], 71), 0),
        "fresh_key_value": draw_fresh_key_value(jax.random.fold_in(key_list[4], 71), 0),
        "lengths": ragged(key_list[3], SEQUENCE_COUNT, 3 * SEQUENCE_COUNT * CACHE_LENGTH // 4, CACHE_LENGTH, 1).astype(jnp.int32),
    }


def one_layer(lengths, items):
    cache, query, fresh = items
    seq_len = cache.shape[2]
    batch = cache.shape[1]
    heads = cache.shape[3] // HEAD_DIM
    blocks = seq_len // BLOCK
    values = cache.astype(jnp.float32).reshape(2, batch, blocks, BLOCK, heads, HEAD_DIM)
    scale = jnp.maximum(lax.optimization_barrier(jnp.max(jnp.abs(values), axis=(3, 5))), 1.0) / 127.0
    quant = (values / scale[:, :, :, None, :, None]).astype(jnp.bfloat16)
    quant = quant.transpose(0, 4, 1, 2, 3, 5).reshape(2, heads * batch, seq_len, HEAD_DIM)
    scale = scale.transpose(0, 3, 1, 2).reshape(2, heads * batch, blocks)
    rows = heads * batch
    inverse = 1.0 / jnp.sqrt(jnp.float32(HEAD_DIM))
    grouped = query.reshape(rows, QUERY_GROUP, HEAD_DIM).astype(jnp.float32)
    raw = jnp.einsum('pgd,prd->pgr', grouped, quant[0].astype(jnp.float32), precision=lax.Precision.HIGHEST)
    scores = raw.reshape(rows, QUERY_GROUP, blocks, BLOCK) * scale[0][:, None, :, None] * inverse
    pair_len = jnp.tile(lengths, heads)
    positions = jnp.arange(seq_len, dtype=jnp.int32).reshape(blocks, BLOCK)
    valid = positions[None] < pair_len[:, None, None]
    masked = jnp.where(valid[:, None], scores, -1e+30)
    peak = lax.optimization_barrier(jnp.max(masked, axis=-1))
    weight = jnp.where(valid[:, None], jnp.exp(masked - peak[..., None]), 0.0)
    total = lax.optimization_barrier(jnp.sum(weight, axis=-1))
    rounded = (weight * scale[1][:, None, :, None]).astype(jnp.bfloat16)
    part = jnp.einsum('pgnt,pntd->pgnd', rounded.astype(jnp.float32), quant[1].reshape(rows, blocks, BLOCK, HEAD_DIM).astype(jnp.float32), precision=lax.Precision.HIGHEST)
    own = jnp.einsum('pgd,pd->pg', grouped, fresh[0].astype(jnp.float32), precision=lax.Precision.HIGHEST) * inverse
    top = jnp.maximum(lax.optimization_barrier(jnp.max(peak, axis=-1)), own)
    scale_factor = jnp.exp(peak - top[..., None])
    own_w = jnp.exp(own - top)
    numer = lax.optimization_barrier(jnp.sum(scale_factor[..., None] * part, axis=2)) + own_w[..., None] * fresh[1].astype(jnp.float32)[:, None, :]
    denom = lax.optimization_barrier(jnp.sum(scale_factor * total, axis=-1)) + own_w
    attended = (numer / denom[..., None]).reshape(rows, QUERY_GROUP * HEAD_DIM).astype(jnp.bfloat16)
    return (quant, scale, attended)

def reference(kv_cache, queries, fresh_key_value, lengths):
    quant, scale, attended = lax.map(lambda items: one_layer(lengths, items), (kv_cache, queries, fresh_key_value))
    return (quant, scale, attended)
```

```python
import jax
import jax.numpy as jnp
from jax import lax
from jax.experimental import pallas as pl
from jax.experimental.pallas import tpu as pltpu
from jax.sharding import PartitionSpec as P

HEAD_DIM = 128
QUERY_GROUP = 8
BLOCK = 128


MESH = pl.DeviceIdType.MESH
Z, X, Y = 8, 4, 2
LAYERS, ROWS = 4, 16


def place():
    index = lax.axis_index("blk")
    return lax.div(index, X * Y), lax.rem(lax.div(index, Y), X), lax.rem(index, Y)


def partner(dz, dx, dy):
    z, x, y = place()
    return lax.rem(z + dz, Z), lax.rem(x + dx, X), lax.rem(y + dy, Y)


def exchange_kernel(cache_ref, out_ref, send_sem, recv_sem):
    z, x, y = place()
    me = (z * X + x) * Y + y

    def each(visit):
        def plane(p, carry):
            dx, dy = lax.div(p, Y), lax.rem(p, Y)
            for i in range(Z - 1):
                visit(i // 2 + 1 if i % 2 == 0 else Z - (i + 1) // 2, dx, dy)
            pl.when(p > 0)(lambda: visit(0, dx, dy))
            return carry

        lax.fori_loop(0, X * Y, plane, 0)

    def piece(ref, layer, pz, px, py):
        pair = 2 * (px * Y + py)
        columns = pl.ds(pl.multiple_of(pz * HEAD_DIM, HEAD_DIM), HEAD_DIM)
        return ref.at[pl.ds(layer, 1), :, pl.ds(pair, 2), :, columns]

    def landing(layer):
        rows = pl.ds(pl.multiple_of(me * ROWS, ROWS), ROWS)
        return out_ref.at[pl.ds(layer, 1), :, :, rows, :]

    barrier = pltpu.get_barrier_semaphore()

    def greet(dz, dx, dy):
        pz, px, py = partner(dz, dx, dy)
        pl.semaphore_signal(
            barrier, inc=1, device_id={"blk": (pz * X + px) * Y + py}, device_id_type=MESH
        )

    each(greet)
    pl.semaphore_wait(barrier, Z * X * Y - 1)

    def layer_sends(layer, carry):
        def send(dz, dx, dy):
            pz, px, py = partner(dz, dx, dy)
            pltpu.make_async_remote_copy(
                src_ref=piece(cache_ref, layer, pz, px, py),
                dst_ref=landing(layer),
                send_sem=send_sem,
                recv_sem=recv_sem,
                device_id={"blk": (pz * X + px) * Y + py},
                device_id_type=MESH,
            ).start()

        each(send)
        pltpu.make_async_copy(piece(cache_ref, layer, z, x, y), landing(layer), recv_sem).start()
        return carry

    lax.fori_loop(0, LAYERS, layer_sends, 0)
    pltpu.make_async_copy(out_ref, out_ref, recv_sem).wait()
    sent = out_ref.at[:, :, :, pl.ds(0, (Z * X * Y - 1) * ROWS), :]
    pltpu.make_async_copy(sent, sent, send_sem).wait()


def exchange(kv_cache):
    return pl.pallas_call(
        exchange_kernel,
        out_shape=jax.ShapeDtypeStruct((LAYERS, 2, 2, Z * X * Y * ROWS, HEAD_DIM), kv_cache.dtype),
        in_specs=[pl.BlockSpec(memory_space=pl.ANY)],
        out_specs=pl.BlockSpec(memory_space=pl.ANY),
        scratch_shapes=[pltpu.SemaphoreType.DMA, pltpu.SemaphoreType.DMA],
        compiler_params=pltpu.CompilerParams(collective_id=0, has_side_effects=True),
    )(kv_cache)


def gathered_once(shard, axis):
    leaves = jax.tree.leaves(shard)
    turns = sorted(range(len(leaves)), key=lambda k: -leaves[k].size)
    width = (1, *leaves[turns[0]].shape)[-1]
    lines = [
        jnp.pad(leaves[k].reshape(-1), (0, -leaves[k].size % width)).reshape(-1, width)
        for k in turns
    ]
    both, at, found = (lax.all_gather(jnp.concatenate(lines), axis), 0, {})
    for k, line in zip(turns, lines):
        piece = both[:, at : at + len(line)].reshape(len(both), -1)
        found[k] = piece[:, : leaves[k].size].reshape(-1, *leaves[k].shape)
        at += len(line)
    numbers = iter(range(len(leaves)))
    return jax.tree.map(lambda _: found[next(numbers)], shard)


def joined(value, axis, join):
    pieces = gathered_once(value, axis)
    head = jax.tree.map(lambda part: part[0], pieces)
    tail = jax.tree.map(lambda part: part[1:], pieces)
    subtotal, _ = lax.scan(lambda subtotal, piece: (join(subtotal, piece), None), head, tail)
    return subtotal


def blend(first_part, second_part):
    peak = jnp.maximum(first_part[0], second_part[0])
    left = jnp.exp(first_part[0] - peak)
    right = jnp.exp(second_part[0] - peak)
    return (
        peak,
        first_part[1] * left + second_part[1] * right,
        first_part[2] * left[..., None] + second_part[2] * right[..., None],
    )


def on_device(kv_cache, queries, fresh_key_value, lengths):
    layers, _, batch, local_rows, width = kv_cache.shape
    heads = width // HEAD_DIM
    blk_count = lax.axis_size("blk")
    blk_place = lax.axis_index("blk")
    pairs_here = heads * batch // blk_count
    seq_rows = local_rows * blk_count
    blocks_here = seq_rows // BLOCK
    pair_start = blk_place * pairs_here
    moved = exchange(kv_cache)
    grouped = moved.reshape(layers, 2, pairs_here, blocks_here, BLOCK, HEAD_DIM)
    block_scale = (
        jnp.maximum(jnp.max(jnp.abs(grouped), axis=(4, 5)).astype(jnp.float32), 1.0) / 127.0
    )
    quant = (grouped.astype(jnp.float32) / block_scale[..., None, None]).astype(jnp.bfloat16)
    quant = quant.reshape(layers, 2, pairs_here, seq_rows, HEAD_DIM)
    seq_start = lax.axis_index("seq") * seq_rows
    pair_len = lax.dynamic_slice_in_dim(jnp.tile(lengths, heads), pair_start, pairs_here)
    positions = seq_start + jnp.arange(seq_rows, dtype=jnp.int32).reshape(blocks_here, BLOCK)
    valid = positions[None] < pair_len[:, None, None]
    inverse = 1.0 / jnp.sqrt(jnp.float32(HEAD_DIM))
    grouped_queries = queries.reshape(layers, pairs_here, QUERY_GROUP, HEAD_DIM)
    peaks = []
    totals = []
    sums = []
    for layer in range(layers):
        raw = jnp.einsum(
            "pgd,prd->pgr",
            grouped_queries[layer],
            quant[layer, 0],
            preferred_element_type=jnp.float32,
        )
        scores = (
            raw.reshape(pairs_here, QUERY_GROUP, blocks_here, BLOCK)
            * block_scale[layer, 0][:, None, :, None]
            * inverse
        )
        masked = jnp.where(valid[:, None], scores, -1e30)
        block_top = jnp.max(masked, axis=-1)
        weight = jnp.where(valid[:, None], jnp.exp(masked - block_top[..., None]), 0.0)
        block_total = jnp.sum(weight, axis=-1)
        rounded = (weight * block_scale[layer, 1][:, None, :, None]).astype(jnp.bfloat16)
        values = quant[layer, 1].reshape(pairs_here, blocks_here, BLOCK, HEAD_DIM)
        block_sum = jnp.einsum(
            "pgnt,pntd->pgnd", rounded, values, preferred_element_type=jnp.float32
        )
        local_top = jnp.max(block_top, axis=-1)
        scale_factor = jnp.exp(block_top - local_top[..., None])
        peaks.append(local_top)
        totals.append(jnp.sum(scale_factor * block_total, axis=-1))
        sums.append(jnp.sum(scale_factor[..., None] * block_sum, axis=2))
    peak = jnp.stack(peaks)
    total = jnp.stack(totals)
    weighted = jnp.stack(sums)
    peak, total, weighted = joined((peak, total, weighted), "seq", blend)
    own = (
        jnp.einsum(
            "lpgd,lpd->lpg",
            grouped_queries,
            fresh_key_value[:, 0],
            preferred_element_type=jnp.float32,
        )
        * inverse
    )
    top = jnp.maximum(peak, own)
    cache_w = jnp.exp(peak - top)
    own_w = jnp.exp(own - top)
    numer = (
        weighted * cache_w[..., None]
        + own_w[..., None] * fresh_key_value[:, 1].astype(jnp.float32)[:, :, None, :]
    )
    denom = total * cache_w + own_w
    attended = (
        (numer / denom[..., None])
        .reshape(layers, pairs_here, QUERY_GROUP * HEAD_DIM)
        .astype(jnp.bfloat16)
    )
    return (quant, block_scale, attended)


def solution(mesh):
    in_specs = (
        P(None, None, None, ("seq", "blk"), None),
        P(None, "blk", None),
        P(None, None, "blk", None),
        P(),
    )
    out_specs = (
        P(None, None, "blk", "seq", None),
        P(None, None, "blk", "seq"),
        P(None, "blk", None),
    )
    return jax.shard_map(
        on_device, mesh=mesh, in_specs=in_specs, out_specs=out_specs, check_vma=False
    )
```
